8 devices in a mesh: dp: 1 (over z), tp2: 2 (over y), tp: 4 (over x, core).
Axes of the slice: x: 2, y: 2, z: 1, core: 2. Of those that a mesh axis runs over, the one named last changes fastest.
Arguments:
- hidden: bfloat16 [512, 1536], P('dp')
- w_gate: bfloat16 [1536, 8960], P(None, ('tp', 'tp2'))
- w_up: bfloat16 [1536, 8960], P(None, ('tp', 'tp2'))
- w_down: bfloat16 [8960, 1536], P('tp', 'tp2')
- norm_gain: float32 [1536], replicated
- w_vocab: bfloat16 [1536, 151936], P('tp2', 'tp')
- temperature: float32 [512], P('dp')
- target: int32 [512], P('dp')
Outputs:
- output 1: float32 [512], P('dp')
- output 2: float32 [512], P('dp')
- output 3: float32 [512], P('dp')
- output 4: bfloat16 [512, 151936], P('dp', ('tp', 'tp2'))
All inputs are finite; a program needn't handle non-finite values.
Results may differ from the reference program's by a relative error of at most 0.00875862.
Values are sent between devices in bfloat16 or wider.
A program may use at most 1 GiB of HBM per device.

```python
import jax
import jax.numpy as jnp
from jax import lax

B = 512
D = 1536
FF = 8960
V = 151936
ROW_BLOCK = 8
NORM_EPS = 1e-6


def setup_inputs(seed: int = 0, part: int = 0) -> dict:
    base_key = jax.random.key(seed)
    shared = jax.random.split(base_key, 5)
    own_keys = jax.random.split(jax.random.fold_in(base_key, part), 5)
    hidden = jax.random.normal(own_keys[0], (B, D), jnp.float32).astype(jnp.bfloat16)
    w_gate = (jax.random.normal(shared[0], (D, FF), jnp.float32) * D ** -0.5).astype(jnp.bfloat16)
    w_up = (jax.random.normal(shared[1], (D, FF), jnp.float32) * D ** -0.5).astype(jnp.bfloat16)
    w_down = (jax.random.normal(shared[2], (FF, D), jnp.float32) * (1.6 * FF ** -0.5)).astype(jnp.bfloat16)
    norm_gain = jax.random.uniform(shared[3], (D,), jnp.float32, 0.5, 1.5)
    w_vocab = (jax.random.normal(shared[4], (D, V), jnp.float32) * (2.5 * D ** -0.5)).astype(jnp.bfloat16)
    temperature = jax.random.uniform(own_keys[1], (B,), jnp.float32, 0.5, 2.0)
    raw_target = jax.random.randint(own_keys[2], (B,), 0, V, jnp.int32)
    first_row = jax.random.randint(own_keys[3], (), 0, B, jnp.int32)
    second_row = (first_row + 1 + jax.random.randint(own_keys[4], (), 0, B - 1, jnp.int32)) % B
    row_ids = jnp.arange(B, dtype=jnp.int32)
    target = jnp.where(row_ids == first_row, 0, jnp.where(row_ids == second_row, V - 1, raw_target)).astype(jnp.int32)
    return {'hidden': hidden, 'w_gate': w_gate, 'w_up': w_up, 'w_down': w_down, 'norm_gain': norm_gain, 'w_vocab': w_vocab, 'temperature': temperature, 'target': target}


def reference(hidden, w_gate, w_up, w_down, norm_gain, w_vocab, temperature, target):
    gate_pre = jnp.dot(hidden, w_gate, preferred_element_type=jnp.float32)
    up_pre = jnp.dot(hidden, w_up, preferred_element_type=jnp.float32)
    act_rows = (jax.nn.silu(gate_pre) * up_pre).astype(jnp.bfloat16)
    y_rows = jnp.dot(act_rows, w_down, preferred_element_type=jnp.float32)
    residual = hidden.astype(jnp.float32) + y_rows
    inv_rms = lax.rsqrt(jnp.mean(residual * residual, axis=1, keepdims=True) + NORM_EPS)
    normed = (norm_gain * residual * inv_rms).astype(jnp.bfloat16)
    num_blocks = B // ROW_BLOCK
    col_ids = jnp.arange(V, dtype=jnp.int32)[None, :]

    def head_block(block_args):
        x_blk, temp_blk, tgt_blk = block_args
        logits = jnp.dot(x_blk, w_vocab, preferred_element_type=jnp.float32) / temp_blk[:, None]
        row_max = jnp.max(logits, axis=1)
        exp_shift = jnp.exp(logits - row_max[:, None])
        sum_exp = jnp.sum(exp_shift, axis=1)
        log_norm = row_max + jnp.log(sum_exp)
        entropy = log_norm - jnp.sum(exp_shift * logits, axis=1) / sum_exp
        tgt_logit = jnp.sum(jnp.where(col_ids == tgt_blk[:, None], logits, 0.0), axis=1)
        logprobs = (logits - log_norm[:, None]).astype(jnp.bfloat16)
        return log_norm, entropy, tgt_logit - log_norm, logprobs

    log_norm, entropy, tgt_logp, logprobs = lax.map(head_block, (normed.reshape(num_blocks, ROW_BLOCK, D), temperature.reshape(num_blocks, ROW_BLOCK), target.reshape(num_blocks, ROW_BLOCK)))
    return (log_norm.reshape(B), entropy.reshape(B), tgt_logp.reshape(B), logprobs.reshape(B, V))
```

```python
import functools

import jax
import jax.numpy as jnp
from jax import lax
from jax.experimental import pallas as pl
from jax.experimental.pallas import tpu as pltpu
from jax.sharding import PartitionSpec as P

NORM_EPS = 1e-6
NEG = float(jnp.finfo(jnp.float32).min)
MESH = pl.DeviceIdType.MESH
CHUNK = 512
SUB = 64
EARLY = 8
DEPTH = 3
BLOCK = 1024


def nt(a, b):
    return lax.dot_general(a, b, (((1,), (1,)), ((), ())), preferred_element_type=jnp.float32)


def tn(a, b):
    return lax.dot_general(a, b, (((0,), (0,)), ((), ())), preferred_element_type=jnp.float32)


def nn(a, b):
    return jnp.dot(a, b, preferred_element_type=jnp.float32)


def head_kernel(n_tp, v_l,
                hidden, wg, wu, wd, gain, temp, target, wv,
                logits, recv,
                hid_v, wg_v, wu_v, wd_v, temp_v, tgt_v, gain_v,
                a_own, a_oth, y_part, y_recv, y_sum, y_oth, x_v, x_t, w_own, w_oth,
                run_m, run_s, run_d, run_t, st_all,
                load_sem, w_send, w_got, a_sem, y_send, y_got, s_sem, x_send, x_got,
                own_sem, oth_sem, st_send, st_got):
    _, rb, d_model = hid_v.shape
    ff_l = wg_v.shape[0]
    d_l = d_model // 2
    rows = n_tp * rb
    n_full = v_l // CHUNK
    rest = v_l - n_full * CHUNK
    tp = lax.axis_index('tp')
    y = lax.axis_index('tp2')
    oy = 1 - y
    me = tp * 2 + y
    other = {'tp2': oy}
    peers = [(dt, dy) for dt in range(n_tp) for dy in range(2) if dt or dy]

    def dev(dt, dy):
        return {'tp': lax.rem(tp + dt, n_tp), 'tp2': lax.rem(y + dy, 2)}

    barrier = pltpu.get_barrier_semaphore()
    for dt, dy in peers:
        pl.semaphore_signal(barrier, inc=1, device_id=dev(dt, dy), device_id_type=MESH)
    pl.semaphore_wait(barrier, len(peers))

    def ship(c, width=CHUNK):
        row = c * CHUNK
        return pltpu.make_async_remote_copy(
            src_ref=wv.at[pl.ds(pl.multiple_of(oy * v_l + row, 16), width), :],
            dst_ref=recv.at[pl.ds(pl.multiple_of(row, 16), width), :],
            send_sem=w_send.at[c], recv_sem=w_got.at[c],
            device_id=other, device_id_type=MESH)

    ship(0).start()

    def load(src, dst, k):
        cp = pltpu.make_async_copy(src, dst, load_sem.at[k])
        cp.start()
        return cp

    own_ff = pl.ds(pl.multiple_of(y * ff_l, 16), ff_l)
    oth_ff = pl.ds(pl.multiple_of(oy * ff_l, 16), ff_l)
    loads = [load(hidden, hid_v, 0), load(wg, wg_v, 1), load(wu, wu_v, 2),
             load(wd.at[own_ff, :], wd_v.at[0], 3), load(wd.at[oth_ff, :], wd_v.at[1], 4),
             load(temp, temp_v, 5), load(target, tgt_v, 6), load(gain, gain_v, 7)]
    for cp in loads:
        cp.wait()

    part = ff_l // 5

    @pl.loop(0, 5)
    def _(j):
        fs = pl.ds(pl.multiple_of(j * part, 16), part)
        h = hid_v[...].reshape(rows, d_model)
        g = nt(wg_v[fs, :], h)
        u = nt(wu_v[fs, :], h)
        a_own[fs, :] = (g * (1.0 / (1.0 + jnp.exp(-g))) * u).astype(jnp.bfloat16)

    a_copy = pltpu.make_async_remote_copy(
        src_ref=a_own, dst_ref=a_oth, send_sem=a_sem.at[0], recv_sem=a_sem.at[1],
        device_id=other, device_id_type=MESH)
    a_copy.start()
    for c in range(1, 4):
        ship(c).start()

    run_m[...] = jnp.full(run_m.shape, NEG, jnp.float32)
    run_s[...] = jnp.zeros(run_s.shape, jnp.float32)
    run_d[...] = jnp.zeros(run_d.shape, jnp.float32)
    run_t[...] = jnp.zeros(run_t.shape, jnp.float32)
    a_copy.wait()

    for q in range(n_tp):
        qs = slice(q * rb, (q + 1) * rb)
        acc = tn(a_own[:, qs], wd_v[0]) + tn(a_oth[:, qs], wd_v[1])
        y_part[q] = acc.astype(jnp.bfloat16)

    y_copies = []
    for o in range(1, n_tp):
        to = lax.rem(tp + o, n_tp)
        cp = pltpu.make_async_remote_copy(
            src_ref=y_part.at[to], dst_ref=y_recv.at[o - 1],
            send_sem=y_send.at[o - 1], recv_sem=y_got.at[o - 1],
            device_id={'tp': to}, device_id_type=MESH)
        cp.start()
        y_copies.append(cp)
    for cp in y_copies:
        cp.wait()
    total = y_part[tp].astype(jnp.float32)
    for o in range(n_tp - 1):
        total += y_recv[o].astype(jnp.float32)
    y_sum[...] = total.astype(jnp.bfloat16)
    s_copy = pltpu.make_async_remote_copy(
        src_ref=y_sum, dst_ref=y_oth, send_sem=s_sem.at[0], recv_sem=s_sem.at[1],
        device_id=other, device_id_type=MESH)
    s_copy.start()
    for c in range(4, EARLY):
        ship(c).start()
    s_copy.wait()

    mine = y_sum[...].astype(jnp.float32)
    theirs = y_oth[...].astype(jnp.float32)
    first = jnp.zeros(mine.shape, jnp.int32) + y == 0
    h = hid_v[tp].astype(jnp.float32)
    r0 = h[:, :d_l] + jnp.where(first, mine, theirs)
    r1 = h[:, d_l:] + jnp.where(first, theirs, mine)
    sq = jnp.sum(r0 * r0, axis=1, keepdims=True) + jnp.sum(r1 * r1, axis=1, keepdims=True)
    inv = lax.rsqrt(sq / d_model + NORM_EPS)
    x_v[tp, :, :d_l] = (gain_v[:, :d_l] * r0 * inv).astype(jnp.bfloat16)
    x_v[tp, :, d_l:] = (gain_v[:, d_l:] * r1 * inv).astype(jnp.bfloat16)
    x_copies = []
    for o in range(1, n_tp):
        to = lax.rem(tp + o, n_tp)
        cp = pltpu.make_async_remote_copy(
            src_ref=x_v.at[tp], dst_ref=x_v.at[tp],
            send_sem=x_send.at[o - 1], recv_sem=x_got.at[o - 1],
            device_id={'tp': to}, device_id_type=MESH)
        cp.start()
        x_copies.append(cp)
    for cp in x_copies:
        cp.wait()
    for q in range(n_tp):
        qs = slice(q * rb, (q + 1) * rb)
        for s in range(2):
            block = x_v[q, :, s * d_l:(s + 1) * d_l].astype(jnp.float32)
            x_t[s, :, qs] = block.T.astype(jnp.bfloat16)

    def own(c, slot, width=CHUNK):
        return pltpu.make_async_copy(
            wv.at[pl.ds(pl.multiple_of(y * v_l + c * CHUNK, 16), width), :],
            w_own.at[slot, pl.ds(0, width), :], own_sem.at[slot])

    def came(c, slot, width=CHUNK):
        return pltpu.make_async_copy(
            recv.at[pl.ds(pl.multiple_of(c * CHUNK, 16), width), :],
            w_oth.at[slot, pl.ds(0, width), :], oth_sem)

    inv_t = 1.0 / temp_v[...]
    local_t = tgt_v[...] - me * v_l

    def update(base, width):
        lg = logits[pl.ds(pl.multiple_of(base, 16), width), :]
        tiles = lg.reshape(width // 8, 8, rows)
        ids = lax.broadcasted_iota(jnp.int32, (width, rows), 0)
        hit = jnp.where(ids == local_t - base, lg, 0.0).reshape(width // 8, 8, rows)
        m_old = run_m[...]
        m_new = jnp.maximum(m_old, jnp.max(tiles, axis=0))
        keep = jnp.exp(m_old - m_new)
        p = jnp.exp(tiles - m_new[None])
        run_m[...] = m_new
        run_s[...] = run_s[...] * keep + jnp.sum(p, axis=0)
        run_d[...] = run_d[...] * keep + jnp.sum(p * tiles, axis=0)
        run_t[...] += jnp.sum(hit, axis=0)

    def multiply(c, slot, width=CHUNK):
        ws = pl.ds(0, width)
        acc = nn(w_own[slot, ws, :], x_t[y]) + nn(w_oth[slot, ws, :], x_t[oy])
        logits[pl.ds(pl.multiple_of(c * CHUNK, 16), width), :] = acc * inv_t

    own(0, 0).start()

    @pl.loop(0, n_full)
    def _(c):
        slot = lax.rem(c, 2)
        after = lax.rem(c + 1, 2)

        @pl.when(c + 1 < n_full)
        def _():
            own(c + 1, after).start()

        @pl.when(c + 1 == n_full)
        def _():
            own(n_full, n_full % 2, rest).start()

        @pl.when((c + DEPTH >= EARLY) & (c + DEPTH < n_full))
        def _():
            ship(c + DEPTH).start()

        @pl.when(c + DEPTH == n_full)
        def _():
            ship(n_full, rest).start()

        own(c, slot).wait()
        ship(c).wait()
        copy = came(c, slot)
        copy.start()
        copy.wait()
        multiply(c, slot)

        @pl.loop(0, CHUNK // SUB)
        def _(k):
            update(c * CHUNK + k * SUB, SUB)

    slot = n_full % 2
    own(n_full, slot, rest).wait()
    ship(n_full, rest).wait()
    copy = came(n_full, slot, rest)
    copy.start()
    copy.wait()
    multiply(n_full, slot, rest)
    update(n_full * CHUNK, rest)

    m = run_m[...]
    top = jnp.max(m, axis=0, keepdims=True)
    keep = jnp.exp(m - top)
    st_all[me, 0:1, :] = top
    st_all[me, 1:2, :] = jnp.sum(run_s[...] * keep, axis=0, keepdims=True)
    st_all[me, 2:3, :] = jnp.sum(run_d[...] * keep, axis=0, keepdims=True)
    st_all[me, 3:4, :] = jnp.sum(run_t[...], axis=0, keepdims=True)
    st_all[me, 4:8, :] = jnp.zeros((4, rows), jnp.float32)
    st_copies = []
    for i, (dt, dy) in enumerate(peers):
        cp = pltpu.make_async_remote_copy(
            src_ref=st_all.at[me], dst_ref=st_all.at[me],
            send_sem=st_send.at[i], recv_sem=st_got.at[i],
            device_id=dev(dt, dy), device_id_type=MESH)
        cp.start()
        st_copies.append(cp)
    for cp in st_copies:
        cp.wait()
    n_dev = n_tp * 2
    g_max = st_all[0, 0:1, :]
    for i in range(1, n_dev):
        g_max = jnp.maximum(g_max, st_all[i, 0:1, :])
    tot_s = jnp.zeros_like(g_max)
    tot_d = jnp.zeros_like(g_max)
    tot_t = jnp.zeros_like(g_max)
    for i in range(n_dev):
        w = jnp.exp(st_all[i, 0:1, :] - g_max)
        tot_s += w * st_all[i, 1:2, :]
        tot_d += w * st_all[i, 2:3, :]
        tot_t += st_all[i, 3:4, :]
    log_norm = g_max + jnp.log(tot_s)
    logits[v_l:v_l + 1, :] = log_norm
    logits[v_l + 1:v_l + 2, :] = log_norm - tot_d / tot_s
    logits[v_l + 2:v_l + 3, :] = tot_t - log_norm
    logits[v_l + 3:v_l + 8, :] = jnp.zeros((5, rows), jnp.float32)


def out_kernel(v_l, logits, out, stats):
    i = pl.program_id(0)
    n_full = v_l // BLOCK
    rest = v_l - n_full * BLOCK

    def put(at, width):
        lg = logits[pl.ds(pl.multiple_of(i * BLOCK + at, 16), width), :]
        out[pl.ds(pl.multiple_of(at, 16), width), :] = (lg - logits[v_l:v_l + 1, :]).astype(jnp.bfloat16)

    @pl.when(i == 0)
    def _():
        stats[...] = logits[v_l:v_l + 8, :]

    @pl.when(i < n_full)
    def _():
        @pl.loop(0, BLOCK // 128)
        def _(k):
            put(k * 128, 128)

    @pl.when(i == n_full)
    def _():
        @pl.loop(0, rest // 112)
        def _(k):
            put(k * 112, 112)


def solution(mesh):
    n_tp = mesh.shape['tp']

    def device_step(hidden, w_gate, w_up, w_down, norm_gain, w_vocab, temperature, target):
        rows, d_model = hidden.shape
        ff_l = w_gate.shape[1]
        d_l = w_down.shape[1]
        v_l = w_vocab.shape[1] // 2
        rb = rows // n_tp
        n_sends = v_l // CHUNK + 1
        any_spec = pl.BlockSpec(memory_space=pl.ANY)
        vmem_spec = pl.BlockSpec(memory_space=pltpu.VMEM)
        bf, f32 = jnp.bfloat16, jnp.float32
        dma = pltpu.SemaphoreType.DMA
        logits, _ = pl.pallas_call(
            functools.partial(head_kernel, n_tp, v_l),
            out_shape=(pltpu.VMEM((v_l + 8, rows), f32),
                       jax.ShapeDtypeStruct((v_l, d_l), bf)),
            in_specs=[any_spec] * 8,
            out_specs=(vmem_spec, any_spec),
            scratch_shapes=[
                pltpu.VMEM((n_tp, rb, d_model), bf),
                pltpu.VMEM((ff_l, d_model), bf),
                pltpu.VMEM((ff_l, d_model), bf),
                pltpu.VMEM((2, ff_l, d_l), bf),
                pltpu.VMEM((1, rows), f32),
                pltpu.VMEM((1, rows), jnp.int32),
                pltpu.VMEM((1, d_model), f32),
                pltpu.VMEM((ff_l, rows), bf),
                pltpu.VMEM((ff_l, rows), bf),
                pltpu.VMEM((n_tp, rb, d_l), bf),
                pltpu.VMEM((n_tp - 1, rb, d_l), bf),
                pltpu.VMEM((rb, d_l), bf),
                pltpu.VMEM((rb, d_l), bf),
                pltpu.VMEM((n_tp, rb, d_model), bf),
                pltpu.VMEM((2, d_l, rows), bf),
                pltpu.VMEM((2, CHUNK, d_l), bf),
                pltpu.VMEM((2, CHUNK, d_l), bf),
                pltpu.VMEM((8, rows), f32),
                pltpu.VMEM((8, rows), f32),
                pltpu.VMEM((8, rows), f32),
                pltpu.VMEM((8, rows), f32),
                pltpu.VMEM((n_tp * 2, 8, rows), f32),
                dma((8,)), dma((n_sends,)), dma((n_sends,)), dma((2,)),
                dma((n_tp - 1,)), dma((n_tp - 1,)), dma((2,)),
                dma((n_tp - 1,)), dma((n_tp - 1,)),
                dma((2,)), dma(()), dma((7,)), dma((7,)),
            ],
            compiler_params=pltpu.CompilerParams(
                collective_id=0, has_side_effects=True, vmem_limit_bytes=25 * 2 ** 20),
        )(hidden.reshape(n_tp, rb, d_model), w_gate.T, w_up.T, w_down, norm_gain.reshape(1, -1),
          temperature.reshape(1, -1), target.reshape(1, -1), w_vocab.T)
        logprobs, stats = pl.pallas_call(
            functools.partial(out_kernel, v_l),
            grid=(pl.cdiv(v_l, BLOCK),),
            out_shape=(pltpu.HBM((v_l, rows), bf), pltpu.HBM((8, rows), f32)),
            in_specs=[vmem_spec],
            out_specs=(pl.BlockSpec((BLOCK, rows), lambda i: (i, 0)), vmem_spec),
            compiler_params=pltpu.CompilerParams(vmem_limit_bytes=8 * 2 ** 20),
        )(logits)
        return stats[0], stats[1], stats[2], logprobs.T

    return jax.shard_map(device_step, mesh=mesh, in_specs=(P('dp', None), P(None, ('tp', 'tp2')), P(None, ('tp', 'tp2')), P('tp', 'tp2'), P(None), P('tp2', 'tp'), P('dp'), P('dp')), out_specs=(P('dp'), P('dp'), P('dp'), P('dp', ('tp', 'tp2'))), check_vma=False)
```

```python
import functools

import jax
import jax.numpy as jnp
from jax import lax
from jax.experimental import pallas as pl
from jax.experimental.pallas import tpu as pltpu
from jax.sharding import PartitionSpec as P

NORM_EPS = 1e-6
NEG = float(jnp.finfo(jnp.float32).min)
MESH = pl.DeviceIdType.MESH
CHUNK = 512
SUB = 64
EARLY = 10
DEPTH = 3
BLOCK = 512
SLOTS = 6


def nt(a, b):
    return lax.dot_general(a, b, (((1,), (1,)), ((), ())), preferred_element_type=jnp.float32)


def tn(a, b):
    return lax.dot_general(a, b, (((0,), (0,)), ((), ())), preferred_element_type=jnp.float32)


def nn(a, b):
    return jnp.dot(a, b, preferred_element_type=jnp.float32)


def head_kernel(n_tp, v_l, ends,
                hidden, wg, wu, wd, gain, temp, target, wv,
                logits, recv,
                hid_v, wg_v, wu_v, wd_v, temp_v, tgt_v, gain_v,
                a_own, a_oth, y_part, y_recv, y_sum, y_oth, x_v, x_t, w_own, w_oth, e_own, e_oth,
                run_m, run_s, run_d, run_t, st_all,
                load_sem, w_send, w_got, a_sem, y_send, y_got, s_sem, x_send, x_got,
                own_sem, oth_sem, end_sem, st_send, st_got):
    _, rb, d_model = hid_v.shape
    ff_l = wg_v.shape[0]
    d_l = d_model // 2
    rows = n_tp * rb
    n_end = sum(ends)
    n_full = (v_l - n_end) // CHUNK
    tp = lax.axis_index('tp')
    y = lax.axis_index('tp2')
    oy = 1 - y
    me = tp * 2 + y
    other = {'tp2': oy}
    peers = [(dt, dy) for dt in range(n_tp) for dy in range(2) if dt or dy]

    def dev(dt, dy):
        return {'tp': lax.rem(tp + dt, n_tp), 'tp2': lax.rem(y + dy, 2)}

    barrier = pltpu.get_barrier_semaphore()
    for dt, dy in peers:
        pl.semaphore_signal(barrier, inc=1, device_id=dev(dt, dy), device_id_type=MESH)
    pl.semaphore_wait(barrier, len(peers))

    def send(row, width, dst, k):
        return pltpu.make_async_remote_copy(
            src_ref=wv.at[pl.ds(pl.multiple_of(oy * v_l + row, 16), width), :],
            dst_ref=dst, send_sem=w_send.at[k], recv_sem=w_got.at[k],
            device_id=other, device_id_type=MESH)

    def ship(c):
        row = c * CHUNK
        return send(row, CHUNK, recv.at[pl.ds(pl.multiple_of(row, 16), CHUNK), :], c)

    def ship_end(i):
        at = sum(ends[:i])
        return send(n_full * CHUNK + at, ends[i], e_oth.at[pl.ds(at, ends[i]), :], n_full + i)

    ship(0).start()
    ship(1).start()

    def load(src, dst, k):
        cp = pltpu.make_async_copy(src, dst, load_sem.at[k])
        cp.start()
        return cp

    own_ff = pl.ds(pl.multiple_of(y * ff_l, 16), ff_l)
    oth_ff = pl.ds(pl.multiple_of(oy * ff_l, 16), ff_l)
    loads = [load(hidden, hid_v, 0), load(wg, wg_v, 1), load(wu, wu_v, 2),
             load(wd.at[own_ff, :], wd_v.at[0], 3), load(wd.at[oth_ff, :], wd_v.at[1], 4),
             load(temp, temp_v, 5), load(target, tgt_v, 6), load(gain, gain_v, 7)]
    for cp in loads:
        cp.wait()

    part = ff_l // 5

    @pl.loop(0, 5)
    def _(j):
        fs = pl.ds(pl.multiple_of(j * part, 16), part)
        h = hid_v[...].reshape(rows, d_model)
        g = nt(wg_v[fs, :], h)
        u = nt(wu_v[fs, :], h)
        a_own[fs, :] = (g * (1.0 / (1.0 + jnp.exp(-g))) * u).astype(jnp.bfloat16)

    a_copy = pltpu.make_async_remote_copy(
        src_ref=a_own, dst_ref=a_oth, send_sem=a_sem.at[0], recv_sem=a_sem.at[1],
        device_id=other, device_id_type=MESH)
    a_copy.start()
    for c in range(2, 6):
        ship(c).start()

    run_m[...] = jnp.full(run_m.shape, NEG, jnp.float32)
    run_s[...] = jnp.zeros(run_s.shape, jnp.float32)
    run_d[...] = jnp.zeros(run_d.shape, jnp.float32)
    run_t[...] = jnp.zeros(run_t.shape, jnp.float32)
    a_copy.wait()

    for q in range(n_tp):
        qs = slice(q * rb, (q + 1) * rb)
        acc = tn(a_own[:, qs], wd_v[0]) + tn(a_oth[:, qs], wd_v[1])
        y_part[q] = acc.astype(jnp.bfloat16)

    y_copies = []
    for o in range(1, n_tp):
        to = lax.rem(tp + o, n_tp)
        cp = pltpu.make_async_remote_copy(
            src_ref=y_part.at[to], dst_ref=y_recv.at[o - 1],
            send_sem=y_send.at[o - 1], recv_sem=y_got.at[o - 1],
            device_id={'tp': to}, device_id_type=MESH)
        cp.start()
        y_copies.append(cp)
    for cp in y_copies:
        cp.wait()
    total = y_part[tp].astype(jnp.float32)
    for o in range(n_tp - 1):
        total += y_recv[o].astype(jnp.float32)
    y_sum[...] = total.astype(jnp.bfloat16)
    s_copy = pltpu.make_async_remote_copy(
        src_ref=y_sum, dst_ref=y_oth, send_sem=s_sem.at[0], recv_sem=s_sem.at[1],
        device_id=other, device_id_type=MESH)
    s_copy.start()
    for c in range(6, EARLY):
        ship(c).start()
    s_copy.wait()

    mine = y_sum[...].astype(jnp.float32)
    theirs = y_oth[...].astype(jnp.float32)
    first = jnp.zeros(mine.shape, jnp.int32) + y == 0
    h = hid_v[tp].astype(jnp.float32)
    r0 = h[:, :d_l] + jnp.where(first, mine, theirs)
    r1 = h[:, d_l:] + jnp.where(first, theirs, mine)
    sq = jnp.sum(r0 * r0, axis=1, keepdims=True) + jnp.sum(r1 * r1, axis=1, keepdims=True)
    inv = lax.rsqrt(sq / d_model + NORM_EPS)
    for k in range(d_model // 128):
        half, at = (r0, k * 128) if k * 128 < d_l else (r1, k * 128 - d_l)
        block = gain_v[k:k + 1, :] * half[:, at:at + 128] * inv
        x_v[tp, :, k * 128:(k + 1) * 128] = block.astype(jnp.bfloat16)
    x_copies = []
    for o in range(1, n_tp):
        to = lax.rem(tp + o, n_tp)
        cp = pltpu.make_async_remote_copy(
            src_ref=x_v.at[tp], dst_ref=x_v.at[tp],
            send_sem=x_send.at[o - 1], recv_sem=x_got.at[o - 1],
            device_id={'tp': to}, device_id_type=MESH)
        cp.start()
        x_copies.append(cp)
    for cp in x_copies:
        cp.wait()
    for q in range(n_tp):
        qs = slice(q * rb, (q + 1) * rb)
        for s in range(2):
            block = x_v[q, :, s * d_l:(s + 1) * d_l].astype(jnp.float32)
            x_t[s, :, qs] = block.T.astype(jnp.bfloat16)

    def own(c, slot):
        return pltpu.make_async_copy(
            wv.at[pl.ds(pl.multiple_of(y * v_l + c * CHUNK, 16), CHUNK), :],
            w_own.at[slot], own_sem.at[slot])

    own_end = pltpu.make_async_copy(
        wv.at[pl.ds(pl.multiple_of(y * v_l + n_full * CHUNK, 16), n_end), :], e_own, end_sem)

    inv_t = 1.0 / temp_v[...]
    local_t = tgt_v[...] - me * v_l

    def update(base, width):
        lg = logits[pl.ds(pl.multiple_of(base, 16), width), :]
        tiles = lg.reshape(width // 8, 8, rows)
        ids = lax.broadcasted_iota(jnp.int32, (width, rows), 0)
        hit = jnp.where(ids == local_t - base, lg, 0.0).reshape(width // 8, 8, rows)
        m_old = run_m[...]
        m_new = jnp.maximum(m_old, jnp.max(tiles, axis=0))
        keep = jnp.exp(m_old - m_new)
        p = jnp.exp(tiles - m_new[None])
        run_m[...] = m_new
        run_s[...] = run_s[...] * keep + jnp.sum(p, axis=0)
        run_d[...] = run_d[...] * keep + jnp.sum(p * tiles, axis=0)
        run_t[...] += jnp.sum(hit, axis=0)

    own_end.start()
    own(0, 0).start()

    @pl.loop(0, n_full)
    def _(c):
        slot = lax.rem(c, 2)

        @pl.when(c + 1 < n_full)
        def _():
            own(c + 1, lax.rem(c + 1, 2)).start()

        @pl.when((c + DEPTH >= EARLY) & (c + DEPTH < n_full))
        def _():
            ship(c + DEPTH).start()

        for i in range(len(ends)):
            @pl.when(c + DEPTH == n_full + i)
            def _():
                ship_end(i).start()

        own(c, slot).wait()
        ship(c).wait()
        came = pltpu.make_async_copy(
            recv.at[pl.ds(pl.multiple_of(c * CHUNK, 16), CHUNK), :], w_oth.at[slot], oth_sem)
        came.start()
        came.wait()
        acc = nn(w_own[slot], x_t[y]) + nn(w_oth[slot], x_t[oy])
        logits[pl.ds(pl.multiple_of(c * CHUNK, 16), CHUNK), :] = acc * inv_t

        @pl.loop(0, CHUNK // SUB)
        def _(k):
            update(c * CHUNK + k * SUB, SUB)

    at = n_full * CHUNK
    own_end.wait()
    logits[at:at + n_end, :] = nn(e_own[...], x_t[y])
    for i, n in enumerate(ends):
        ship_end(i).wait()
        es = slice(at - n_full * CHUNK, at - n_full * CHUNK + n)
        logits[at:at + n, :] = (logits[at:at + n, :] + nn(e_oth[es, :], x_t[oy])) * inv_t
        steps = -(-n // 128)
        for k in range(steps):
            update(at + k * (n // steps), n // steps)
        at += n

    m = run_m[...]
    top = jnp.max(m, axis=0, keepdims=True)
    keep = jnp.exp(m - top)
    st_all[me, 0:1, :] = top
    st_all[me, 1:2, :] = jnp.sum(run_s[...] * keep, axis=0, keepdims=True)
    st_all[me, 2:3, :] = jnp.sum(run_d[...] * keep, axis=0, keepdims=True)
    st_all[me, 3:4, :] = jnp.sum(run_t[...], axis=0, keepdims=True)
    st_all[me, 4:8, :] = jnp.zeros((4, rows), jnp.float32)
    st_copies = []
    for i, (dt, dy) in enumerate(peers):
        cp = pltpu.make_async_remote_copy(
            src_ref=st_all.at[me], dst_ref=st_all.at[me],
            send_sem=st_send.at[i], recv_sem=st_got.at[i],
            device_id=dev(dt, dy), device_id_type=MESH)
        cp.start()
        st_copies.append(cp)
    for cp in st_copies:
        cp.wait()
    n_dev = n_tp * 2
    g_max = st_all[0, 0:1, :]
    for i in range(1, n_dev):
        g_max = jnp.maximum(g_max, st_all[i, 0:1, :])
    tot_s = jnp.zeros_like(g_max)
    tot_d = jnp.zeros_like(g_max)
    tot_t = jnp.zeros_like(g_max)
    for i in range(n_dev):
        w = jnp.exp(st_all[i, 0:1, :] - g_max)
        tot_s += w * st_all[i, 1:2, :]
        tot_d += w * st_all[i, 2:3, :]
        tot_t += st_all[i, 3:4, :]
    log_norm = g_max + jnp.log(tot_s)
    logits[v_l:v_l + 1, :] = log_norm
    logits[v_l + 1:v_l + 2, :] = log_norm - tot_d / tot_s
    logits[v_l + 2:v_l + 3, :] = tot_t - log_norm
    logits[v_l + 3:v_l + 8, :] = jnp.zeros((5, rows), jnp.float32)


def out_kernel(v_l, logits, out, log_norm, entropy, target_lp, buf, row0, row1, row2, sem, row_sem):
    n_full = v_l // BLOCK
    rest = v_l - n_full * BLOCK
    row_copies = []
    for k, (row, dst) in enumerate(((row0, log_norm), (row1, entropy), (row2, target_lp))):
        row[...] = logits[v_l + k:v_l + k + 1, :]
        cp = pltpu.make_async_copy(row, dst, row_sem.at[k])
        cp.start()
        row_copies.append(cp)

    def put(b, slot, width=BLOCK):
        return pltpu.make_async_copy(
            buf.at[slot, pl.ds(0, width), :],
            out.at[pl.ds(pl.multiple_of(b * BLOCK, 16), width), :], sem.at[slot])

    def fill(b, slot, width=BLOCK):
        lg = logits[pl.ds(pl.multiple_of(b * BLOCK, 16), width), :]
        buf[slot, :width, :] = (lg - row0[...]).astype(jnp.bfloat16)

    @pl.loop(0, n_full)
    def _(b):
        slot = lax.rem(b, SLOTS)

        @pl.when(b >= SLOTS)
        def _():
            put(b - SLOTS, slot).wait()

        fill(b, slot)
        put(b, slot).start()

    slot = n_full % SLOTS
    put(n_full - SLOTS, slot).wait()
    fill(n_full, slot, rest)
    put(n_full, slot, rest).start()
    for b in range(n_full - SLOTS + 1, n_full):
        put(b, b % SLOTS).wait()
    put(n_full, slot, rest).wait()
    for cp in row_copies:
        cp.wait()


def solution(mesh):
    n_tp = mesh.shape['tp']

    def device_step(hidden, w_gate, w_up, w_down, norm_gain, w_vocab, temperature, target):
        rows, d_model = hidden.shape
        ff_l = w_gate.shape[1]
        d_l = w_down.shape[1]
        v_l = w_vocab.shape[1] // 2
        rb = rows // n_tp
        over = v_l % CHUNK + CHUNK
        ends = (over - 224, 160, 64)
        n_sends = v_l // CHUNK - 1 + len(ends)
        any_spec = pl.BlockSpec(memory_space=pl.ANY)
        vmem_spec = pl.BlockSpec(memory_space=pltpu.VMEM)
        bf, f32 = jnp.bfloat16, jnp.float32
        dma = pltpu.SemaphoreType.DMA
        logits, _ = pl.pallas_call(
            functools.partial(head_kernel, n_tp, v_l, ends),
            out_shape=(pltpu.VMEM((v_l + 8, rows), f32),
                       jax.ShapeDtypeStruct((v_l, d_l), bf)),
            in_specs=[any_spec] * 8,
            out_specs=(vmem_spec, any_spec),
            scratch_shapes=[
                pltpu.VMEM((n_tp, rb, d_model), bf),
                pltpu.VMEM((ff_l, d_model), bf),
                pltpu.VMEM((ff_l, d_model), bf),
                pltpu.VMEM((2, ff_l, d_l), bf),
                pltpu.VMEM((1, rows), f32),
                pltpu.VMEM((1, rows), jnp.int32),
                pltpu.VMEM((d_model // 128, 128), f32),
                pltpu.VMEM((ff_l, rows), bf),
                pltpu.VMEM((ff_l, rows), bf),
                pltpu.VMEM((n_tp, rb, d_l), bf),
                pltpu.VMEM((n_tp - 1, rb, d_l), bf),
                pltpu.VMEM((rb, d_l), bf),
                pltpu.VMEM((rb, d_l), bf),
                pltpu.VMEM((n_tp, rb, d_model), bf),
                pltpu.VMEM((2, d_l, rows), bf),
                pltpu.VMEM((2, CHUNK, d_l), bf),
                pltpu.VMEM((2, CHUNK, d_l), bf),
                pltpu.VMEM((over, d_l), bf),
                pltpu.VMEM((over, d_l), bf),
                pltpu.VMEM((8, rows), f32),
                pltpu.VMEM((8, rows), f32),
                pltpu.VMEM((8, rows), f32),
                pltpu.VMEM((8, rows), f32),
                pltpu.VMEM((n_tp * 2, 8, rows), f32),
                dma((8,)), dma((n_sends,)), dma((n_sends,)), dma((2,)),
                dma((n_tp - 1,)), dma((n_tp - 1,)), dma((2,)),
                dma((n_tp - 1,)), dma((n_tp - 1,)),
                dma((2,)), dma(()), dma(()), dma((7,)), dma((7,)),
            ],
            compiler_params=pltpu.CompilerParams(
                collective_id=0, has_side_effects=True, vmem_limit_bytes=25 * 2 ** 20),
        )(hidden.reshape(n_tp, rb, d_model), w_gate.T, w_up.T, w_down, norm_gain.reshape(-1, 128),
          temperature.reshape(1, -1), target.reshape(1, -1), w_vocab.T)
        row = pltpu.HBM((1, rows), f32)
        logprobs, log_norm, entropy, target_lp = pl.pallas_call(
            functools.partial(out_kernel, v_l),
            out_shape=(pltpu.HBM((v_l, rows), bf), row, row, row),
            in_specs=[vmem_spec],
            out_specs=(any_spec,) * 4,
            scratch_shapes=[pltpu.VMEM((SLOTS, BLOCK, rows), bf)] + [pltpu.VMEM((1, rows), f32)] * 3 + [
                dma((SLOTS,)), dma((3,))],
            compiler_params=pltpu.CompilerParams(vmem_limit_bytes=8 * 2 ** 20),
        )(logits)
        return log_norm.reshape(rows), entropy.reshape(rows), target_lp.reshape(rows), logprobs.T

    return jax.shard_map(device_step, mesh=mesh, in_specs=(P('dp', None), P(None, ('tp', 'tp2')), P(None, ('tp', 'tp2')), P('tp', 'tp2'), P(None), P('tp2', 'tp'), P('dp'), P('dp')), out_specs=(P('dp'), P('dp'), P('dp'), P('dp', ('tp', 'tp2'))), check_vma=False)
```

```python
import functools

import jax
import jax.numpy as jnp
from jax import lax
from jax.experimental import pallas as pl
from jax.experimental.pallas import tpu as pltpu
from jax.sharding import PartitionSpec as P

NORM_EPS = 1e-6
NEG = float(jnp.finfo(jnp.float32).min)
MESH = pl.DeviceIdType.MESH
CHUNK = 512
SUB = 64
EARLY = 12
DEPTH = 3
BLOCK = 512
SLOTS = 6


def nt(a, b):
    return lax.dot_general(a, b, (((1,), (1,)), ((), ())), preferred_element_type=jnp.float32)


def tn(a, b):
    return lax.dot_general(a, b, (((0,), (0,)), ((), ())), preferred_element_type=jnp.float32)


def nn(a, b):
    return jnp.dot(a, b, preferred_element_type=jnp.float32)


def head_kernel(n_tp, v_l, ends,
                hidden, wg, wu, wd, gain, temp, target, wv,
                logits, recv,
                hid_v, wg_v, wu_v, wd_v, temp_v, tgt_v, gain_v,
                a_own, a_oth, y_part, y_recv, y_sum, y_oth, x_v, x_t, w_own, w_oth, e_own, e_oth,
                run_m, run_s, run_d, run_t, st_all,
                load_sem, w_send, w_got, a_sem, y_send, y_got, s_sem, x_send, x_got,
                own_sem, oth_sem, end_sem, st_send, st_got):
    _, rb, d_model = hid_v.shape
    ff_l = wg_v.shape[0]
    d_l = d_model // 2
    rows = n_tp * rb
    n_end = sum(ends)
    n_full = (v_l - n_end) // CHUNK
    tp = lax.axis_index('tp')
    y = lax.axis_index('tp2')
    oy = 1 - y
    me = tp * 2 + y
    other = {'tp2': oy}
    peers = [(dt, dy) for dt in range(n_tp) for dy in range(2) if dt or dy]

    def dev(dt, dy):
        return {'tp': lax.rem(tp + dt, n_tp), 'tp2': lax.rem(y + dy, 2)}

    def load(src, dst, k):
        cp = pltpu.make_async_copy(src, dst, load_sem.at[k])
        cp.start()
        return cp

    own_ff = pl.ds(pl.multiple_of(y * ff_l, 16), ff_l)
    oth_ff = pl.ds(pl.multiple_of(oy * ff_l, 16), ff_l)
    loads = [load(hidden, hid_v, 0), load(wg, wg_v, 1), load(wu, wu_v, 2),
             load(wd.at[own_ff, :], wd_v.at[0], 3), load(wd.at[oth_ff, :], wd_v.at[1], 4),
             load(temp, temp_v, 5), load(target, tgt_v, 6), load(gain, gain_v, 7)]

    barrier = pltpu.get_barrier_semaphore()
    for dt, dy in peers:
        pl.semaphore_signal(barrier, inc=1, device_id=dev(dt, dy), device_id_type=MESH)
    pl.semaphore_wait(barrier, len(peers))

    def send(row, width, dst, k):
        return pltpu.make_async_remote_copy(
            src_ref=wv.at[pl.ds(pl.multiple_of(oy * v_l + row, 16), width), :],
            dst_ref=dst, send_sem=w_send.at[k], recv_sem=w_got.at[k],
            device_id=other, device_id_type=MESH)

    def ship(c):
        row = c * CHUNK
        return send(row, CHUNK, recv.at[pl.ds(pl.multiple_of(row, 16), CHUNK), :], c)

    def ship_end(i):
        at = sum(ends[:i])
        return send(n_full * CHUNK + at, ends[i], e_oth.at[pl.ds(at, ends[i]), :], n_full + i)

    for c in range(4):
        ship(c).start()

    ship(0).wait()
    for cp in loads:
        cp.wait()

    part = ff_l // 5

    @pl.loop(0, 5)
    def _(j):
        fs = pl.ds(pl.multiple_of(j * part, 16), part)
        h = hid_v[...].reshape(rows, d_model)
        g = nt(wg_v[fs, :], h)
        u = nt(wu_v[fs, :], h)
        a_own[fs, :] = (g * (1.0 / (1.0 + jnp.exp(-g))) * u).astype(jnp.bfloat16)

    a_copy = pltpu.make_async_remote_copy(
        src_ref=a_own, dst_ref=a_oth, send_sem=a_sem.at[0], recv_sem=a_sem.at[1],
        device_id=other, device_id_type=MESH)
    a_copy.start()
    for c in range(4, 8):
        ship(c).start()

    run_m[...] = jnp.full(run_m.shape, NEG, jnp.float32)
    run_s[...] = jnp.zeros(run_s.shape, jnp.float32)
    run_d[...] = jnp.zeros(run_d.shape, jnp.float32)
    run_t[...] = jnp.zeros(run_t.shape, jnp.float32)
    a_copy.wait()

    for q in range(n_tp):
        qs = slice(q * rb, (q + 1) * rb)
        acc = tn(a_own[:, qs], wd_v[0]) + tn(a_oth[:, qs], wd_v[1])
        y_part[q] = acc.astype(jnp.bfloat16)

    y_copies = []
    for o in range(1, n_tp):
        to = lax.rem(tp + o, n_tp)
        cp = pltpu.make_async_remote_copy(
            src_ref=y_part.at[to], dst_ref=y_recv.at[o - 1],
            send_sem=y_send.at[o - 1], recv_sem=y_got.at[o - 1],
            device_id={'tp': to}, device_id_type=MESH)
        cp.start()
        y_copies.append(cp)
    for cp in y_copies:
        cp.wait()
    total = y_part[tp].astype(jnp.float32)
    for o in range(n_tp - 1):
        total += y_recv[o].astype(jnp.float32)
    y_sum[...] = total.astype(jnp.bfloat16)
    s_copy = pltpu.make_async_remote_copy(
        src_ref=y_sum, dst_ref=y_oth, send_sem=s_sem.at[0], recv_sem=s_sem.at[1],
        device_id=other, device_id_type=MESH)
    s_copy.start()
    for c in range(8, EARLY):
        ship(c).start()
    s_copy.wait()

    mine = y_sum[...].astype(jnp.float32)
    theirs = y_oth[...].astype(jnp.float32)
    first = jnp.zeros(mine.shape, jnp.int32) + y == 0
    h = hid_v[tp].astype(jnp.float32)
    r0 = h[:, :d_l] + jnp.where(first, mine, theirs)
    r1 = h[:, d_l:] + jnp.where(first, theirs, mine)
    sq = jnp.sum(r0 * r0, axis=1, keepdims=True) + jnp.sum(r1 * r1, axis=1, keepdims=True)
    inv = lax.rsqrt(sq / d_model + NORM_EPS)
    for k in range(d_model // 128):
        half, at = (r0, k * 128) if k * 128 < d_l else (r1, k * 128 - d_l)
        block = gain_v[k:k + 1, :] * half[:, at:at + 128] * inv
        x_v[tp, :, k * 128:(k + 1) * 128] = block.astype(jnp.bfloat16)
    x_copies = []
    for o in range(1, n_tp):
        to = lax.rem(tp + o, n_tp)
        cp = pltpu.make_async_remote_copy(
            src_ref=x_v.at[tp], dst_ref=x_v.at[tp],
            send_sem=x_send.at[o - 1], recv_sem=x_got.at[o - 1],
            device_id={'tp': to}, device_id_type=MESH)
        cp.start()
        x_copies.append(cp)
    for cp in x_copies:
        cp.wait()
    for q in range(n_tp):
        qs = slice(q * rb, (q + 1) * rb)
        for s in range(2):
            block = x_v[q, :, s * d_l:(s + 1) * d_l].astype(jnp.float32)
            x_t[s, :, qs] = block.T.astype(jnp.bfloat16)

    def own(c, slot):
        return pltpu.make_async_copy(
            wv.at[pl.ds(pl.multiple_of(y * v_l + c * CHUNK, 16), CHUNK), :],
            w_own.at[slot], own_sem.at[slot])

    own_end = pltpu.make_async_copy(
        wv.at[pl.ds(pl.multiple_of(y * v_l + n_full * CHUNK, 16), n_end), :], e_own, end_sem)

    inv_t = 1.0 / temp_v[...]
    local_t = tgt_v[...] - me * v_l

    def update(base, width):
        lg = logits[pl.ds(pl.multiple_of(base, 16), width), :]
        tiles = lg.reshape(width // 8, 8, rows)
        ids = lax.broadcasted_iota(jnp.int32, (width, rows), 0)
        hit = jnp.where(ids == local_t - base, lg, 0.0).reshape(width // 8, 8, rows)
        m_old = run_m[...]
        m_new = jnp.maximum(m_old, jnp.max(tiles, axis=0))
        keep = jnp.exp(m_old - m_new)
        p = jnp.exp(tiles - m_new[None])
        run_m[...] = m_new
        run_s[...] = run_s[...] * keep + jnp.sum(p, axis=0)
        run_d[...] = run_d[...] * keep + jnp.sum(p * tiles, axis=0)
        run_t[...] += jnp.sum(hit, axis=0)

    def came(c, slot):
        return pltpu.make_async_copy(
            recv.at[pl.ds(pl.multiple_of(c * CHUNK, 16), CHUNK), :], w_oth.at[slot], oth_sem.at[slot])

    def compute(c, slot):
        own(c, slot).wait()
        came(c, slot).wait()
        acc = nn(w_own[slot], x_t[y]) + nn(w_oth[slot], x_t[oy])
        logits[pl.ds(pl.multiple_of(c * CHUNK, 16), CHUNK), :] = acc * inv_t

        @pl.loop(0, CHUNK // SUB)
        def _(k):
            update(c * CHUNK + k * SUB, SUB)

    own_end.start()

    @pl.loop(0, n_full)
    def _(c):
        slot = lax.rem(c, 2)
        own(c, slot).start()

        @pl.when((c + DEPTH >= EARLY) & (c + DEPTH < n_full))
        def _():
            ship(c + DEPTH).start()

        for i in range(len(ends)):
            @pl.when(c + DEPTH == n_full + i)
            def _():
                ship_end(i).start()

        @pl.when(c > 0)
        def _():
            ship(c).wait()

        came(c, slot).start()

        @pl.when(c > 0)
        def _():
            compute(c - 1, lax.rem(c + 1, 2))

    compute(n_full - 1, (n_full - 1) % 2)
    at = n_full * CHUNK
    own_end.wait()
    logits[at:at + n_end, :] = nn(e_own[...], x_t[y])
    for i, n in enumerate(ends):
        ship_end(i).wait()
        es = slice(at - n_full * CHUNK, at - n_full * CHUNK + n)
        logits[at:at + n, :] = (logits[at:at + n, :] + nn(e_oth[es, :], x_t[oy])) * inv_t
        steps = -(-n // 128)
        for k in range(steps):
            update(at + k * (n // steps), n // steps)
        at += n

    m = run_m[...]
    top = jnp.max(m, axis=0, keepdims=True)
    keep = jnp.exp(m - top)
    st_all[me, 0:1, :] = top
    st_all[me, 1:2, :] = jnp.sum(run_s[...] * keep, axis=0, keepdims=True)
    st_all[me, 2:3, :] = jnp.sum(run_d[...] * keep, axis=0, keepdims=True)
    st_all[me, 3:4, :] = jnp.sum(run_t[...], axis=0, keepdims=True)
    st_copies = []
    for i, (dt, dy) in enumerate(peers):
        cp = pltpu.make_async_remote_copy(
            src_ref=st_all.at[me], dst_ref=st_all.at[me],
            send_sem=st_send.at[i], recv_sem=st_got.at[i],
            device_id=dev(dt, dy), device_id_type=MESH)
        cp.start()
        st_copies.append(cp)
    for cp in st_copies:
        cp.wait()
    n_dev = n_tp * 2
    g_max = st_all[0, 0:1, :]
    for i in range(1, n_dev):
        g_max = jnp.maximum(g_max, st_all[i, 0:1, :])
    tot_s = jnp.zeros_like(g_max)
    tot_d = jnp.zeros_like(g_max)
    tot_t = jnp.zeros_like(g_max)
    for i in range(n_dev):
        w = jnp.exp(st_all[i, 0:1, :] - g_max)
        tot_s += w * st_all[i, 1:2, :]
        tot_d += w * st_all[i, 2:3, :]
        tot_t += st_all[i, 3:4, :]
    log_norm = g_max + jnp.log(tot_s)
    logits[v_l:v_l + 1, :] = log_norm
    logits[v_l + 1:v_l + 2, :] = log_norm - tot_d / tot_s
    logits[v_l + 2:v_l + 3, :] = tot_t - log_norm
    logits[v_l + 3:v_l + 8, :] = jnp.zeros((5, rows), jnp.float32)


def out_kernel(v_l, logits, out, log_norm, entropy, target_lp, buf, row0, row1, row2, sem, row_sem):
    n_full = v_l // BLOCK
    rest = v_l - n_full * BLOCK
    row_copies = []
    for k, (row, dst) in enumerate(((row0, log_norm), (row1, entropy), (row2, target_lp))):
        row[...] = logits[v_l + k:v_l + k + 1, :]
        cp = pltpu.make_async_copy(row, dst, row_sem.at[k])
        cp.start()
        row_copies.append(cp)

    def put(b, slot, width=BLOCK):
        return pltpu.make_async_copy(
            buf.at[slot, pl.ds(0, width), :],
            out.at[pl.ds(pl.multiple_of(b * BLOCK, 16), width), :], sem.at[slot])

    def fill(b, slot, width=BLOCK):
        lg = logits[pl.ds(pl.multiple_of(b * BLOCK, 16), width), :]
        buf[slot, :width, :] = (lg - row0[...]).astype(jnp.bfloat16)

    @pl.loop(0, n_full)
    def _(b):
        slot = lax.rem(b, SLOTS)

        @pl.when(b >= SLOTS)
        def _():
            put(b - SLOTS, slot).wait()

        fill(b, slot)
        put(b, slot).start()

    slot = n_full % SLOTS
    put(n_full - SLOTS, slot).wait()
    fill(n_full, slot, rest)
    put(n_full, slot, rest).start()
    for b in range(n_full - SLOTS + 1, n_full):
        put(b, b % SLOTS).wait()
    put(n_full, slot, rest).wait()
    for cp in row_copies:
        cp.wait()


def solution(mesh):
    n_tp = mesh.shape['tp']

    def device_step(hidden, w_gate, w_up, w_down, norm_gain, w_vocab, temperature, target):
        rows, d_model = hidden.shape
        ff_l = w_gate.shape[1]
        d_l = w_down.shape[1]
        v_l = w_vocab.shape[1] // 2
        rb = rows // n_tp
        over = v_l % CHUNK + CHUNK
        ends = (over - 224, 160, 64)
        n_sends = v_l // CHUNK - 1 + len(ends)
        any_spec = pl.BlockSpec(memory_space=pl.ANY)
        vmem_spec = pl.BlockSpec(memory_space=pltpu.VMEM)
        bf, f32 = jnp.bfloat16, jnp.float32
        dma = pltpu.SemaphoreType.DMA
        logits, _ = pl.pallas_call(
            functools.partial(head_kernel, n_tp, v_l, ends),
            out_shape=(pltpu.VMEM((v_l + 8, rows), f32),
                       jax.ShapeDtypeStruct((v_l, d_l), bf)),
            in_specs=[any_spec] * 8,
            out_specs=(vmem_spec, any_spec),
            scratch_shapes=[
                pltpu.VMEM((n_tp, rb, d_model), bf),
                pltpu.VMEM((ff_l, d_model), bf),
                pltpu.VMEM((ff_l, d_model), bf),
                pltpu.VMEM((2, ff_l, d_l), bf),
                pltpu.VMEM((1, rows), f32),
                pltpu.VMEM((1, rows), jnp.int32),
                pltpu.VMEM((d_model // 128, 128), f32),
                pltpu.VMEM((ff_l, rows), bf),
                pltpu.VMEM((ff_l, rows), bf),
                pltpu.VMEM((n_tp, rb, d_l), bf),
                pltpu.VMEM((n_tp - 1, rb, d_l), bf),
                pltpu.VMEM((rb, d_l), bf),
                pltpu.VMEM((rb, d_l), bf),
                pltpu.VMEM((n_tp, rb, d_model), bf),
                pltpu.VMEM((2, d_l, rows), bf),
                pltpu.VMEM((2, CHUNK, d_l), bf),
                pltpu.VMEM((2, CHUNK, d_l), bf),
                pltpu.VMEM((over, d_l), bf),
                pltpu.VMEM((over, d_l), bf),
                pltpu.VMEM((8, rows), f32),
                pltpu.VMEM((8, rows), f32),
                pltpu.VMEM((8, rows), f32),
                pltpu.VMEM((8, rows), f32),
                pltpu.VMEM((n_tp * 2, 4, rows), f32),
                dma((8,)), dma((n_sends,)), dma((n_sends,)), dma((2,)),
                dma((n_tp - 1,)), dma((n_tp - 1,)), dma((2,)),
                dma((n_tp - 1,)), dma((n_tp - 1,)),
                dma((2,)), dma((2,)), dma(()), dma((7,)), dma((7,)),
            ],
            compiler_params=pltpu.CompilerParams(
                collective_id=0, has_side_effects=True, vmem_limit_bytes=25 * 2 ** 20),
        )(hidden.reshape(n_tp, rb, d_model), w_gate.T, w_up.T, w_down, norm_gain.reshape(-1, 128),
          temperature.reshape(1, -1), target.reshape(1, -1), w_vocab.T)
        row = pltpu.HBM((1, rows), f32)
        logprobs, log_norm, entropy, target_lp = pl.pallas_call(
            functools.partial(out_kernel, v_l),
            out_shape=(pltpu.HBM((v_l, rows), bf), row, row, row),
            in_specs=[vmem_spec],
            out_specs=(any_spec,) * 4,
            scratch_shapes=[pltpu.VMEM((SLOTS, BLOCK, rows), bf)] + [pltpu.VMEM((1, rows), f32)] * 3 + [
                dma((SLOTS,)), dma((3,))],
            compiler_params=pltpu.CompilerParams(vmem_limit_bytes=8 * 2 ** 20),
        )(logits)
        return log_norm.reshape(rows), entropy.reshape(rows), target_lp.reshape(rows), logprobs.T

    return jax.shard_map(device_step, mesh=mesh, in_specs=(P('dp', None), P(None, ('tp', 'tp2')), P(None, ('tp', 'tp2')), P('tp', 'tp2'), P(None), P('tp2', 'tp'), P('dp'), P('dp')), out_specs=(P('dp'), P('dp'), P('dp'), P('dp', ('tp', 'tp2'))), check_vma=False)
```

```python
import functools

import jax
import jax.numpy as jnp
from jax import lax
from jax.experimental import pallas as pl
from jax.experimental.pallas import tpu as pltpu
from jax.sharding import PartitionSpec as P

NORM_EPS = 1e-6
NEG = float(jnp.finfo(jnp.float32).min)
MESH = pl.DeviceIdType.MESH
CHUNK = 512
SUB = 64
EARLY = 12
DEPTH = 3
BLOCK = 512
SLOTS = 6


def nt(a, b):
    return lax.dot_general(a, b, (((1,), (1,)), ((), ())), preferred_element_type=jnp.float32)


def tn(a, b):
    return lax.dot_general(a, b, (((0,), (0,)), ((), ())), preferred_element_type=jnp.float32)


def nn(a, b):
    return jnp.dot(a, b, preferred_element_type=jnp.float32)


def head_kernel(n_tp, v_l, ends,
                hidden, wg, wu, wd, gain, temp, target, wv,
                logits, recv,
                hid_v, wg_v, wu_v, wd_v, temp_v, tgt_v, gain_v,
                a_own, a_oth, y_part, y_recv, y_sum, y_oth, x_v, x_t, w_own, w_oth, e_own, e_oth,
                run_m, run_s, run_d, run_t, st_all,
                load_sem, w_send, w_got, a_sem, y_send, y_got, s_sem, x_send, x_got,
                own_sem, oth_sem, end_sem, st_send, st_got):
    _, rb, d_model = hid_v.shape
    ff_l = wg_v.shape[0]
    d_l = d_model // 2
    rows = n_tp * rb
    n_end = sum(ends)
    n_full = (v_l - n_end) // CHUNK
    tp = lax.axis_index('tp')
    y = lax.axis_index('tp2')
    oy = 1 - y
    me = tp * 2 + y
    other = {'tp2': oy}
    peers = [(dt, dy) for dt in range(n_tp) for dy in range(2) if dt or dy]

    def dev(dt, dy):
        return {'tp': lax.rem(tp + dt, n_tp), 'tp2': lax.rem(y + dy, 2)}

    def load(src, dst, k):
        cp = pltpu.make_async_copy(src, dst, load_sem.at[k])
        cp.start()
        return cp

    own_ff = pl.ds(pl.multiple_of(y * ff_l, 16), ff_l)
    oth_ff = pl.ds(pl.multiple_of(oy * ff_l, 16), ff_l)
    loads = [load(hidden, hid_v, 0), load(wg, wg_v, 1), load(wu, wu_v, 2),
             load(wd.at[own_ff, :], wd_v.at[0], 3), load(wd.at[oth_ff, :], wd_v.at[1], 4),
             load(temp, temp_v, 5), load(target, tgt_v, 6), load(gain, gain_v, 7)]

    barrier = pltpu.get_barrier_semaphore()
    near = [(dt, dy) for dt, dy in peers if not dt or not dy]
    for dt, dy in near:
        pl.semaphore_signal(barrier, inc=1, device_id=dev(dt, dy), device_id_type=MESH)
    pl.semaphore_wait(barrier, len(near))

    def send(row, width, dst, k):
        return pltpu.make_async_remote_copy(
            src_ref=wv.at[pl.ds(pl.multiple_of(oy * v_l + row, 16), width), :],
            dst_ref=dst, send_sem=w_send.at[k], recv_sem=w_got.at[k],
            device_id=other, device_id_type=MESH)

    def ship(c):
        row = c * CHUNK
        return send(row, CHUNK, recv.at[pl.ds(pl.multiple_of(row, 16), CHUNK), :], c)

    def ship_end(i):
        at = sum(ends[:i])
        return send(n_full * CHUNK + at, ends[i], e_oth.at[pl.ds(at, ends[i]), :], n_full + i)

    for c in range(4):
        ship(c).start()

    ship(0).wait()
    for cp in loads:
        cp.wait()

    part = ff_l // 5

    @pl.loop(0, 5)
    def _(j):
        fs = pl.ds(pl.multiple_of(j * part, 16), part)
        h = hid_v[...].reshape(rows, d_model)
        g = nt(wg_v[fs, :], h)
        u = nt(wu_v[fs, :], h)
        a_own[fs, :] = (g * (1.0 / (1.0 + jnp.exp(-g))) * u).astype(jnp.bfloat16)

    a_copy = pltpu.make_async_remote_copy(
        src_ref=a_own, dst_ref=a_oth, send_sem=a_sem.at[0], recv_sem=a_sem.at[1],
        device_id=other, device_id_type=MESH)
    a_copy.start()
    for c in range(4, 8):
        ship(c).start()

    run_m[...] = jnp.full(run_m.shape, NEG, jnp.float32)
    run_s[...] = jnp.zeros(run_s.shape, jnp.float32)
    run_d[...] = jnp.zeros(run_d.shape, jnp.float32)
    run_t[...] = jnp.zeros(run_t.shape, jnp.float32)
    a_copy.wait()

    for q in range(n_tp):
        qs = slice(q * rb, (q + 1) * rb)
        acc = tn(a_own[:, qs], wd_v[0]) + tn(a_oth[:, qs], wd_v[1])
        y_part[q] = acc.astype(jnp.bfloat16)

    y_copies = []
    for o in range(1, n_tp):
        to = lax.rem(tp + o, n_tp)
        cp = pltpu.make_async_remote_copy(
            src_ref=y_part.at[to], dst_ref=y_recv.at[o - 1],
            send_sem=y_send.at[o - 1], recv_sem=y_got.at[o - 1],
            device_id={'tp': to}, device_id_type=MESH)
        cp.start()
        y_copies.append(cp)
    for cp in y_copies:
        cp.wait()
    total = y_part[tp].astype(jnp.float32)
    for o in range(n_tp - 1):
        total += y_recv[o].astype(jnp.float32)
    y_sum[...] = total.astype(jnp.bfloat16)
    s_copy = pltpu.make_async_remote_copy(
        src_ref=y_sum, dst_ref=y_oth, send_sem=s_sem.at[0], recv_sem=s_sem.at[1],
        device_id=other, device_id_type=MESH)
    s_copy.start()
    for c in range(8, EARLY):
        ship(c).start()
    s_copy.wait()

    mine = y_sum[...].astype(jnp.float32)
    theirs = y_oth[...].astype(jnp.float32)
    first = jnp.zeros(mine.shape, jnp.int32) + y == 0
    h = hid_v[tp].astype(jnp.float32)
    r0 = h[:, :d_l] + jnp.where(first, mine, theirs)
    r1 = h[:, d_l:] + jnp.where(first, theirs, mine)
    sq = jnp.sum(r0 * r0, axis=1, keepdims=True) + jnp.sum(r1 * r1, axis=1, keepdims=True)
    inv = lax.rsqrt(sq / d_model + NORM_EPS)
    for k in range(d_model // 128):
        half, at = (r0, k * 128) if k * 128 < d_l else (r1, k * 128 - d_l)
        block = gain_v[k:k + 1, :] * half[:, at:at + 128] * inv
        x_v[tp, :, k * 128:(k + 1) * 128] = block.astype(jnp.bfloat16)
    x_copies = []
    for o in range(1, n_tp):
        to = lax.rem(tp + o, n_tp)
        cp = pltpu.make_async_remote_copy(
            src_ref=x_v.at[tp], dst_ref=x_v.at[tp],
            send_sem=x_send.at[o - 1], recv_sem=x_got.at[o - 1],
            device_id={'tp': to}, device_id_type=MESH)
        cp.start()
        x_copies.append(cp)
    for cp in x_copies:
        cp.wait()
    for q in range(n_tp):
        qs = slice(q * rb, (q + 1) * rb)
        for s in range(2):
            block = x_v[q, :, s * d_l:(s + 1) * d_l].astype(jnp.float32)
            x_t[s, :, qs] = block.T.astype(jnp.bfloat16)

    def own(c, slot):
        return pltpu.make_async_copy(
            wv.at[pl.ds(pl.multiple_of(y * v_l + c * CHUNK, 16), CHUNK), :],
            w_own.at[slot], own_sem.at[slot])

    own_end = pltpu.make_async_copy(
        wv.at[pl.ds(pl.multiple_of(y * v_l + n_full * CHUNK, 16), n_end), :], e_own, end_sem)

    inv_t = 1.0 / temp_v[...]
    local_t = tgt_v[...] - me * v_l

    def update(base, width):
        lg = logits[pl.ds(pl.multiple_of(base, 16), width), :]
        tiles = lg.reshape(width // 8, 8, rows)
        ids = lax.broadcasted_iota(jnp.int32, (width, rows), 0)
        hit = jnp.where(ids == local_t - base, lg, 0.0).reshape(width // 8, 8, rows)
        m_old = run_m[...]
        m_new = jnp.maximum(m_old, jnp.max(tiles, axis=0))
        keep = jnp.exp(m_old - m_new)
        p = jnp.exp(tiles - m_new[None])
        run_m[...] = m_new
        run_s[...] = run_s[...] * keep + jnp.sum(p, axis=0)
        run_d[...] = run_d[...] * keep + jnp.sum(p * tiles, axis=0)
        run_t[...] += jnp.sum(hit, axis=0)

    def came(c, slot):
        return pltpu.make_async_copy(
            recv.at[pl.ds(pl.multiple_of(c * CHUNK, 16), CHUNK), :], w_oth.at[slot], oth_sem.at[slot])

    def compute(c, slot):
        own(c, slot).wait()
        came(c, slot).wait()
        acc = nn(w_own[slot], x_t[y]) + nn(w_oth[slot], x_t[oy])
        logits[pl.ds(pl.multiple_of(c * CHUNK, 16), CHUNK), :] = acc * inv_t

        @pl.loop(0, CHUNK // SUB)
        def _(k):
            update(c * CHUNK + k * SUB, SUB)

    own_end.start()

    @pl.loop(0, n_full)
    def _(c):
        slot = lax.rem(c, 2)
        own(c, slot).start()

        @pl.when((c + DEPTH >= EARLY) & (c + DEPTH < n_full))
        def _():
            ship(c + DEPTH).start()

        for i in range(len(ends)):
            @pl.when(c + DEPTH == n_full + i)
            def _():
                ship_end(i).start()

        @pl.when(c > 0)
        def _():
            ship(c).wait()

        came(c, slot).start()

        @pl.when(c > 0)
        def _():
            compute(c - 1, lax.rem(c + 1, 2))

    compute(n_full - 1, (n_full - 1) % 2)
    at = n_full * CHUNK
    own_end.wait()
    logits[at:at + n_end, :] = nn(e_own[...], x_t[y])
    for i, n in enumerate(ends):
        ship_end(i).wait()
        es = slice(at - n_full * CHUNK, at - n_full * CHUNK + n)
        logits[at:at + n, :] = (logits[at:at + n, :] + nn(e_oth[es, :], x_t[oy])) * inv_t
        steps = -(-n // 128)
        for k in range(steps):
            update(at + k * (n // steps), n // steps)
        at += n

    m = run_m[...]
    top = jnp.max(m, axis=0, keepdims=True)
    keep = jnp.exp(m - top)
    st_all[me, 0:1, :] = top
    st_all[me, 1:2, :] = jnp.sum(run_s[...] * keep, axis=0, keepdims=True)
    st_all[me, 2:3, :] = jnp.sum(run_d[...] * keep, axis=0, keepdims=True)
    st_all[me, 3:4, :] = jnp.sum(run_t[...], axis=0, keepdims=True)
    st_copies = []
    for i, (dt, dy) in enumerate(peers):
        cp = pltpu.make_async_remote_copy(
            src_ref=st_all.at[me], dst_ref=st_all.at[me],
            send_sem=st_send.at[i], recv_sem=st_got.at[i],
            device_id=dev(dt, dy), device_id_type=MESH)
        cp.start()
        st_copies.append(cp)
    for cp in st_copies:
        cp.wait()
    n_dev = n_tp * 2
    g_max = st_all[0, 0:1, :]
    for i in range(1, n_dev):
        g_max = jnp.maximum(g_max, st_all[i, 0:1, :])
    tot_s = jnp.zeros_like(g_max)
    tot_d = jnp.zeros_like(g_max)
    tot_t = jnp.zeros_like(g_max)
    for i in range(n_dev):
        w = jnp.exp(st_all[i, 0:1, :] - g_max)
        tot_s += w * st_all[i, 1:2, :]
        tot_d += w * st_all[i, 2:3, :]
        tot_t += st_all[i, 3:4, :]
    log_norm = g_max + jnp.log(tot_s)
    logits[v_l:v_l + 1, :] = log_norm
    logits[v_l + 1:v_l + 2, :] = log_norm - tot_d / tot_s
    logits[v_l + 2:v_l + 3, :] = tot_t - log_norm
    logits[v_l + 3:v_l + 8, :] = jnp.zeros((5, rows), jnp.float32)


def out_kernel(v_l, logits, out, log_norm, entropy, target_lp, buf, row0, row1, row2, sem, row_sem):
    n_full = v_l // BLOCK
    rest = v_l - n_full * BLOCK
    row_copies = []
    for k, (row, dst) in enumerate(((row0, log_norm), (row1, entropy), (row2, target_lp))):
        row[...] = logits[v_l + k:v_l + k + 1, :]
        cp = pltpu.make_async_copy(row, dst, row_sem.at[k])
        cp.start()
        row_copies.append(cp)

    def put(b, slot, width=BLOCK):
        return pltpu.make_async_copy(
            buf.at[slot, pl.ds(0, width), :],
            out.at[pl.ds(pl.multiple_of(b * BLOCK, 16), width), :], sem.at[slot])

    def fill(b, slot, width=BLOCK):
        lg = logits[pl.ds(pl.multiple_of(b * BLOCK, 16), width), :]
        buf[slot, :width, :] = (lg - row0[...]).astype(jnp.bfloat16)

    @pl.loop(0, n_full)
    def _(b):
        slot = lax.rem(b, SLOTS)

        @pl.when(b >= SLOTS)
        def _():
            put(b - SLOTS, slot).wait()

        fill(b, slot)
        put(b, slot).start()

    slot = n_full % SLOTS
    put(n_full - SLOTS, slot).wait()
    fill(n_full, slot, rest)
    put(n_full, slot, rest).start()
    for b in range(n_full - SLOTS + 1, n_full):
        put(b, b % SLOTS).wait()
    put(n_full, slot, rest).wait()
    for cp in row_copies:
        cp.wait()


def solution(mesh):
    n_tp = mesh.shape['tp']

    def device_step(hidden, w_gate, w_up, w_down, norm_gain, w_vocab, temperature, target):
        rows, d_model = hidden.shape
        ff_l = w_gate.shape[1]
        d_l = w_down.shape[1]
        v_l = w_vocab.shape[1] // 2
        rb = rows // n_tp
        over = v_l % CHUNK + CHUNK
        ends = (over - 224, 160, 64)
        n_sends = v_l // CHUNK - 1 + len(ends)
        any_spec = pl.BlockSpec(memory_space=pl.ANY)
        vmem_spec = pl.BlockSpec(memory_space=pltpu.VMEM)
        bf, f32 = jnp.bfloat16, jnp.float32
        dma = pltpu.SemaphoreType.DMA
        logits, _ = pl.pallas_call(
            functools.partial(head_kernel, n_tp, v_l, ends),
            out_shape=(pltpu.VMEM((v_l + 8, rows), f32),
                       jax.ShapeDtypeStruct((v_l, d_l), bf)),
            in_specs=[any_spec] * 8,
            out_specs=(vmem_spec, any_spec),
            scratch_shapes=[
                pltpu.VMEM((n_tp, rb, d_model), bf),
                pltpu.VMEM((ff_l, d_model), bf),
                pltpu.VMEM((ff_l, d_model), bf),
                pltpu.VMEM((2, ff_l, d_l), bf),
                pltpu.VMEM((1, rows), f32),
                pltpu.VMEM((1, rows), jnp.int32),
                pltpu.VMEM((d_model // 128, 128), f32),
                pltpu.VMEM((ff_l, rows), bf),
                pltpu.VMEM((ff_l, rows), bf),
                pltpu.VMEM((n_tp, rb, d_l), bf),
                pltpu.VMEM((n_tp - 1, rb, d_l), bf),
                pltpu.VMEM((rb, d_l), bf),
                pltpu.VMEM((rb, d_l), bf),
                pltpu.VMEM((n_tp, rb, d_model), bf),
                pltpu.VMEM((2, d_l, rows), bf),
                pltpu.VMEM((2, CHUNK, d_l), bf),
                pltpu.VMEM((2, CHUNK, d_l), bf),
                pltpu.VMEM((over, d_l), bf),
                pltpu.VMEM((over, d_l), bf),
                pltpu.VMEM((8, rows), f32),
                pltpu.VMEM((8, rows), f32),
                pltpu.VMEM((8, rows), f32),
                pltpu.VMEM((8, rows), f32),
                pltpu.VMEM((n_tp * 2, 4, rows), f32),
                dma((8,)), dma((n_sends,)), dma((n_sends,)), dma((2,)),
                dma((n_tp - 1,)), dma((n_tp - 1,)), dma((2,)),
                dma((n_tp - 1,)), dma((n_tp - 1,)),
                dma((2,)), dma((2,)), dma(()), dma((7,)), dma((7,)),
            ],
            compiler_params=pltpu.CompilerParams(
                collective_id=0, has_side_effects=True, vmem_limit_bytes=25 * 2 ** 20),
        )(hidden.reshape(n_tp, rb, d_model), w_gate.T, w_up.T, w_down, norm_gain.reshape(-1, 128),
          temperature.reshape(1, -1), target.reshape(1, -1), w_vocab.T)
        row = pltpu.HBM((1, rows), f32)
        logprobs, log_norm, entropy, target_lp = pl.pallas_call(
            functools.partial(out_kernel, v_l),
            out_shape=(pltpu.HBM((v_l, rows), bf), row, row, row),
            in_specs=[vmem_spec],
            out_specs=(any_spec,) * 4,
            scratch_shapes=[pltpu.VMEM((SLOTS, BLOCK, rows), bf)] + [pltpu.VMEM((1, rows), f32)] * 3 + [
                dma((SLOTS,)), dma((3,))],
            compiler_params=pltpu.CompilerParams(vmem_limit_bytes=8 * 2 ** 20),
        )(logits)
        return log_norm.reshape(rows), entropy.reshape(rows), target_lp.reshape(rows), logprobs.T

    return jax.shard_map(device_step, mesh=mesh, in_specs=(P('dp', None), P(None, ('tp', 'tp2')), P(None, ('tp', 'tp2')), P('tp', 'tp2'), P(None), P('tp2', 'tp'), P('dp'), P('dp')), out_specs=(P('dp'), P('dp'), P('dp'), P('dp', ('tp', 'tp2'))), check_vma=False)
```

```python
import functools

import jax
import jax.numpy as jnp
from jax import lax
from jax.experimental import pallas as pl
from jax.experimental.pallas import tpu as pltpu
from jax.sharding import PartitionSpec as P

NORM_EPS = 1e-6
NEG = float(jnp.finfo(jnp.float32).min)
MESH = pl.DeviceIdType.MESH
CHUNK = 512
SUB = 64
EARLY = 12
DEPTH = 3
BLOCK = 512
SLOTS = 6


def nt(a, b):
    return lax.dot_general(a, b, (((1,), (1,)), ((), ())), preferred_element_type=jnp.float32)


def tn(a, b):
    return lax.dot_general(a, b, (((0,), (0,)), ((), ())), preferred_element_type=jnp.float32)


def nn(a, b):
    return jnp.dot(a, b, preferred_element_type=jnp.float32)


def head_kernel(n_tp, v_l, ends,
                hidden, wg, wu, wd, gain, temp, target, wv,
                logits, recv,
                hid_v, wg_v, wu_v, wd_v, temp_v, tgt_v, gain_v,
                a_own, a_oth, y_part, y_recv, y_sum, y_oth, x_v, x_t, w_own, w_oth, e_own, e_oth,
                run_m, run_s, run_d, run_t, st_all,
                load_sem, w_send, w_got, a_sem, y_send, y_got, s_sem, x_send, x_got,
                own_sem, oth_sem, end_sem, st_send, st_got):
    _, rb, d_model = hid_v.shape
    ff_l = wg_v.shape[0]
    d_l = d_model // 2
    rows = n_tp * rb
    n_end = sum(ends)
    n_full = (v_l - n_end) // CHUNK
    tp = lax.axis_index('tp')
    y = lax.axis_index('tp2')
    oy = 1 - y
    me = tp * 2 + y
    other = {'tp2': oy}
    peers = [(dt, dy) for dt in range(n_tp) for dy in range(2) if dt or dy]

    def dev(dt, dy):
        return {'tp': lax.rem(tp + dt, n_tp), 'tp2': lax.rem(y + dy, 2)}

    def load(src, dst, k):
        cp = pltpu.make_async_copy(src, dst, load_sem.at[k])
        cp.start()
        return cp

    own_ff = pl.ds(pl.multiple_of(y * ff_l, 16), ff_l)
    oth_ff = pl.ds(pl.multiple_of(oy * ff_l, 16), ff_l)
    loads = [load(hidden, hid_v, 0), load(wg, wg_v, 1), load(wu, wu_v, 2),
             load(wd.at[own_ff, :], wd_v.at[0], 3), load(wd.at[oth_ff, :], wd_v.at[1], 4),
             load(temp, temp_v, 5), load(target, tgt_v, 6), load(gain, gain_v, 7)]

    barrier = pltpu.get_barrier_semaphore()
    near = [(dt, dy) for dt, dy in peers if not dt or not dy]
    for dt, dy in near:
        pl.semaphore_signal(barrier, inc=1, device_id=dev(dt, dy), device_id_type=MESH)
    pl.semaphore_wait(barrier, len(near))

    def send(row, width, dst, k):
        return pltpu.make_async_remote_copy(
            src_ref=wv.at[pl.ds(pl.multiple_of(oy * v_l + row, 16), width), :],
            dst_ref=dst, send_sem=w_send.at[k], recv_sem=w_got.at[k],
            device_id=other, device_id_type=MESH)

    def ship(c):
        row = c * CHUNK
        return send(row, CHUNK, recv.at[pl.ds(pl.multiple_of(row, 16), CHUNK), :], c)

    def ship_end(i):
        at = sum(ends[:i])
        return send(n_full * CHUNK + at, ends[i], e_oth.at[pl.ds(at, ends[i]), :], n_full + i)

    for c in range(4):
        ship(c).start()

    ship(0).wait()
    for cp in loads:
        cp.wait()

    part = ff_l // 5

    @pl.loop(0, 5)
    def _(j):
        fs = pl.ds(pl.multiple_of(j * part, 16), part)
        h = hid_v[...].reshape(rows, d_model)
        g = nt(wg_v[fs, :], h)
        u = nt(wu_v[fs, :], h)
        a_own[fs, :] = (g * (1.0 / (1.0 + jnp.exp(-g))) * u).astype(jnp.bfloat16)

    a_copy = pltpu.make_async_remote_copy(
        src_ref=a_own, dst_ref=a_oth, send_sem=a_sem.at[0], recv_sem=a_sem.at[1],
        device_id=other, device_id_type=MESH)
    a_copy.start()
    for c in range(4, 8):
        ship(c).start()

    run_m[...] = jnp.full(run_m.shape, NEG, jnp.float32)
    run_s[...] = jnp.zeros(run_s.shape, jnp.float32)
    run_d[...] = jnp.zeros(run_d.shape, jnp.float32)
    run_t[...] = jnp.zeros(run_t.shape, jnp.float32)
    a_copy.wait()

    for q in range(n_tp):
        qs = slice(q * rb, (q + 1) * rb)
        acc = tn(a_own[:, qs], wd_v[0]) + tn(a_oth[:, qs], wd_v[1])
        y_part[q] = acc.astype(jnp.bfloat16)

    y_copies = []
    for o in range(1, n_tp):
        to = lax.rem(tp + o, n_tp)
        cp = pltpu.make_async_remote_copy(
            src_ref=y_part.at[to], dst_ref=y_recv.at[o - 1],
            send_sem=y_send.at[o - 1], recv_sem=y_got.at[o - 1],
            device_id={'tp': to}, device_id_type=MESH)
        cp.start()
        y_copies.append(cp)
    for cp in y_copies:
        cp.wait()
    total = y_part[tp].astype(jnp.float32)
    for o in range(n_tp - 1):
        total += y_recv[o].astype(jnp.float32)
    y_sum[...] = total.astype(jnp.bfloat16)
    s_copy = pltpu.make_async_remote_copy(
        src_ref=y_sum, dst_ref=y_oth, send_sem=s_sem.at[0], recv_sem=s_sem.at[1],
        device_id=other, device_id_type=MESH)
    s_copy.start()
    for c in range(8, EARLY):
        ship(c).start()
    s_copy.wait()

    mine = y_sum[...].astype(jnp.float32)
    theirs = y_oth[...].astype(jnp.float32)
    first = jnp.zeros(mine.shape, jnp.int32) + y == 0
    h = hid_v[tp].astype(jnp.float32)
    r0 = h[:, :d_l] + jnp.where(first, mine, theirs)
    r1 = h[:, d_l:] + jnp.where(first, theirs, mine)
    sq = jnp.sum(r0 * r0, axis=1, keepdims=True) + jnp.sum(r1 * r1, axis=1, keepdims=True)
    inv = lax.rsqrt(sq / d_model + NORM_EPS)
    for k in range(d_model // 128):
        half, at = (r0, k * 128) if k * 128 < d_l else (r1, k * 128 - d_l)
        block = gain_v[k:k + 1, :] * half[:, at:at + 128] * inv
        x_v[tp, :, k * 128:(k + 1) * 128] = block.astype(jnp.bfloat16)
    x_copies = []
    for o in range(1, n_tp):
        to = lax.rem(tp + o, n_tp)
        cp = pltpu.make_async_remote_copy(
            src_ref=x_v.at[tp], dst_ref=x_v.at[tp],
            send_sem=x_send.at[o - 1], recv_sem=x_got.at[o - 1],
            device_id={'tp': to}, device_id_type=MESH)
        cp.start()
        x_copies.append(cp)
    for cp in x_copies:
        cp.wait()
    for q in range(n_tp):
        qs = slice(q * rb, (q + 1) * rb)
        for s in range(2):
            block = x_v[q, :, s * d_l:(s + 1) * d_l].astype(jnp.float32)
            x_t[s, :, qs] = block.T.astype(jnp.bfloat16)

    def own(c, slot):
        return pltpu.make_async_copy(
            wv.at[pl.ds(pl.multiple_of(y * v_l + c * CHUNK, 16), CHUNK), :],
            w_own.at[slot], own_sem.at[slot])

    own_end = pltpu.make_async_copy(
        wv.at[pl.ds(pl.multiple_of(y * v_l + n_full * CHUNK, 16), n_end), :], e_own, end_sem)

    inv_t = 1.0 / temp_v[...]
    local_t = tgt_v[...] - me * v_l

    def update(base, width):
        lg = logits[pl.ds(pl.multiple_of(base, 16), width), :]
        tiles = lg.reshape(width // 8, 8, rows)
        ids = lax.broadcasted_iota(jnp.int32, (width, rows), 0)
        hit = jnp.where(ids == local_t - base, lg, 0.0).reshape(width // 8, 8, rows)
        m_old = run_m[...]
        m_new = jnp.maximum(m_old, jnp.max(tiles, axis=0))
        keep = jnp.exp(m_old - m_new)
        p = jnp.exp(tiles - m_new[None])
        run_m[...] = m_new
        run_s[...] = run_s[...] * keep + jnp.sum(p, axis=0)
        run_d[...] = run_d[...] * keep + jnp.sum(p * tiles, axis=0)
        run_t[...] += jnp.sum(hit, axis=0)

    def came(c, slot):
        return pltpu.make_async_copy(
            recv.at[pl.ds(pl.multiple_of(c * CHUNK, 16), CHUNK), :], w_oth.at[slot], oth_sem.at[slot])

    def compute(c, slot):
        own(c, slot).wait()
        came(c, slot).wait()
        acc = nn(w_own[slot], x_t[y]) + nn(w_oth[slot], x_t[oy])
        logits[pl.ds(pl.multiple_of(c * CHUNK, 16), CHUNK), :] = acc * inv_t

        @pl.loop(0, CHUNK // SUB)
        def _(k):
            update(c * CHUNK + k * SUB, SUB)

    own_end.start()

    @pl.loop(0, n_full)
    def _(c):
        slot = lax.rem(c, 2)
        own(c, slot).start()

        @pl.when((c + DEPTH >= EARLY) & (c + DEPTH < n_full))
        def _():
            ship(c + DEPTH).start()

        for i in range(len(ends)):
            @pl.when(c + DEPTH == n_full + i)
            def _():
                ship_end(i).start()

        @pl.when(c > 0)
        def _():
            ship(c).wait()

        came(c, slot).start()

        @pl.when(c > 0)
        def _():
            compute(c - 1, lax.rem(c + 1, 2))

    compute(n_full - 1, (n_full - 1) % 2)
    at = n_full * CHUNK
    own_end.wait()
    logits[at:at + n_end, :] = nn(e_own[...], x_t[y])
    for i, n in enumerate(ends):
        ship_end(i).wait()
        es = slice(at - n_full * CHUNK, at - n_full * CHUNK + n)
        logits[at:at + n, :] = (logits[at:at + n, :] + nn(e_oth[es, :], x_t[oy])) * inv_t
        steps = -(-n // 128)
        for k in range(steps):
            update(at + k * (n // steps), n // steps)
        at += n

    m = run_m[...]
    top = jnp.max(m, axis=0, keepdims=True)
    keep = jnp.exp(m - top)
    st_all[me, 0:1, :] = top
    st_all[me, 1:2, :] = jnp.sum(run_s[...] * keep, axis=0, keepdims=True)
    st_all[me, 2:3, :] = jnp.sum(run_d[...] * keep, axis=0, keepdims=True)
    st_all[me, 3:4, :] = jnp.sum(run_t[...], axis=0, keepdims=True)
    st_copies = []
    for i, (dt, dy) in enumerate(sorted(peers, key=lambda p: -(p[0] > 0) - p[1])):
        cp = pltpu.make_async_remote_copy(
            src_ref=st_all.at[me], dst_ref=st_all.at[me],
            send_sem=st_send.at[i], recv_sem=st_got.at[i],
            device_id=dev(dt, dy), device_id_type=MESH)
        cp.start()
        st_copies.append(cp)
    for cp in st_copies:
        cp.wait()
    n_dev = n_tp * 2
    g_max = st_all[0, 0:1, :]
    for i in range(1, n_dev):
        g_max = jnp.maximum(g_max, st_all[i, 0:1, :])
    tot_s = jnp.zeros_like(g_max)
    tot_d = jnp.zeros_like(g_max)
    tot_t = jnp.zeros_like(g_max)
    for i in range(n_dev):
        w = jnp.exp(st_all[i, 0:1, :] - g_max)
        tot_s += w * st_all[i, 1:2, :]
        tot_d += w * st_all[i, 2:3, :]
        tot_t += st_all[i, 3:4, :]
    log_norm = g_max + jnp.log(tot_s)
    logits[v_l:v_l + 1, :] = log_norm
    logits[v_l + 1:v_l + 2, :] = log_norm - tot_d / tot_s
    logits[v_l + 2:v_l + 3, :] = tot_t - log_norm
    logits[v_l + 3:v_l + 8, :] = jnp.zeros((5, rows), jnp.float32)


def out_kernel(v_l, logits, out, log_norm, entropy, target_lp, buf, row0, row1, row2, sem, row_sem):
    n_full = v_l // BLOCK
    rest = v_l - n_full * BLOCK
    row_copies = []
    for k, (row, dst) in enumerate(((row0, log_norm), (row1, entropy), (row2, target_lp))):
        row[...] = logits[v_l + k:v_l + k + 1, :]
        cp = pltpu.make_async_copy(row, dst, row_sem.at[k])
        cp.start()
        row_copies.append(cp)

    def put(b, slot, width=BLOCK):
        return pltpu.make_async_copy(
            buf.at[slot, pl.ds(0, width), :],
            out.at[pl.ds(pl.multiple_of(b * BLOCK, 16), width), :], sem.at[slot])

    def fill(b, slot, width=BLOCK):
        lg = logits[pl.ds(pl.multiple_of(b * BLOCK, 16), width), :]
        buf[slot, :width, :] = (lg - row0[...]).astype(jnp.bfloat16)

    @pl.loop(0, n_full)
    def _(b):
        slot = lax.rem(b, SLOTS)

        @pl.when(b >= SLOTS)
        def _():
            put(b - SLOTS, slot).wait()

        fill(b, slot)
        put(b, slot).start()

    slot = n_full % SLOTS
    put(n_full - SLOTS, slot).wait()
    fill(n_full, slot, rest)
    put(n_full, slot, rest).start()
    for b in range(n_full - SLOTS + 1, n_full):
        put(b, b % SLOTS).wait()
    put(n_full, slot, rest).wait()
    for cp in row_copies:
        cp.wait()


def solution(mesh):
    n_tp = mesh.shape['tp']

    def device_step(hidden, w_gate, w_up, w_down, norm_gain, w_vocab, temperature, target):
        rows, d_model = hidden.shape
        ff_l = w_gate.shape[1]
        d_l = w_down.shape[1]
        v_l = w_vocab.shape[1] // 2
        rb = rows // n_tp
        over = v_l % CHUNK + CHUNK
        ends = (over - 224, 160, 64)
        n_sends = v_l // CHUNK - 1 + len(ends)
        any_spec = pl.BlockSpec(memory_space=pl.ANY)
        vmem_spec = pl.BlockSpec(memory_space=pltpu.VMEM)
        bf, f32 = jnp.bfloat16, jnp.float32
        dma = pltpu.SemaphoreType.DMA
        logits, _ = pl.pallas_call(
            functools.partial(head_kernel, n_tp, v_l, ends),
            out_shape=(pltpu.VMEM((v_l + 8, rows), f32),
                       jax.ShapeDtypeStruct((v_l, d_l), bf)),
            in_specs=[any_spec] * 8,
            out_specs=(vmem_spec, any_spec),
            scratch_shapes=[
                pltpu.VMEM((n_tp, rb, d_model), bf),
                pltpu.VMEM((ff_l, d_model), bf),
                pltpu.VMEM((ff_l, d_model), bf),
                pltpu.VMEM((2, ff_l, d_l), bf),
                pltpu.VMEM((1, rows), f32),
                pltpu.VMEM((1, rows), jnp.int32),
                pltpu.VMEM((d_model // 128, 128), f32),
                pltpu.VMEM((ff_l, rows), bf),
                pltpu.VMEM((ff_l, rows), bf),
                pltpu.VMEM((n_tp, rb, d_l), bf),
                pltpu.VMEM((n_tp - 1, rb, d_l), bf),
                pltpu.VMEM((rb, d_l), bf),
                pltpu.VMEM((rb, d_l), bf),
                pltpu.VMEM((n_tp, rb, d_model), bf),
                pltpu.VMEM((2, d_l, rows), bf),
                pltpu.VMEM((2, CHUNK, d_l), bf),
                pltpu.VMEM((2, CHUNK, d_l), bf),
                pltpu.VMEM((over, d_l), bf),
                pltpu.VMEM((over, d_l), bf),
                pltpu.VMEM((8, rows), f32),
                pltpu.VMEM((8, rows), f32),
                pltpu.VMEM((8, rows), f32),
                pltpu.VMEM((8, rows), f32),
                pltpu.VMEM((n_tp * 2, 4, rows), f32),
                dma((8,)), dma((n_sends,)), dma((n_sends,)), dma((2,)),
                dma((n_tp - 1,)), dma((n_tp - 1,)), dma((2,)),
                dma((n_tp - 1,)), dma((n_tp - 1,)),
                dma((2,)), dma((2,)), dma(()), dma((7,)), dma((7,)),
            ],
            compiler_params=pltpu.CompilerParams(
                collective_id=0, has_side_effects=True, vmem_limit_bytes=25 * 2 ** 20),
        )(hidden.reshape(n_tp, rb, d_model), w_gate.T, w_up.T, w_down, norm_gain.reshape(-1, 128),
          temperature.reshape(1, -1), target.reshape(1, -1), w_vocab.T)
        row = pltpu.HBM((1, rows), f32)
        logprobs, log_norm, entropy, target_lp = pl.pallas_call(
            functools.partial(out_kernel, v_l),
            out_shape=(pltpu.HBM((v_l, rows), bf), row, row, row),
            in_specs=[vmem_spec],
            out_specs=(any_spec,) * 4,
            scratch_shapes=[pltpu.VMEM((SLOTS, BLOCK, rows), bf)] + [pltpu.VMEM((1, rows), f32)] * 3 + [
                dma((SLOTS,)), dma((3,))],
            compiler_params=pltpu.CompilerParams(vmem_limit_bytes=8 * 2 ** 20),
        )(logits)
        return log_norm.reshape(rows), entropy.reshape(rows), target_lp.reshape(rows), logprobs.T

    return jax.shard_map(device_step, mesh=mesh, in_specs=(P('dp', None), P(None, ('tp', 'tp2')), P(None, ('tp', 'tp2')), P('tp', 'tp2'), P(None), P('tp2', 'tp'), P('dp'), P('dp')), out_specs=(P('dp'), P('dp'), P('dp'), P('dp', ('tp', 'tp2'))), check_vma=False)
```
